512 devices in a mesh: dom: 512 (over z, y, x, core).
Axes of the slice: x: 4, y: 4, z: 16, core: 2. Of those that a mesh axis runs over, the one named last changes fastest.
Arguments:
- particles: float32 [512, 2, 256, 128], P('dom'), may hold values from -60 to 60
- offspring: int32 [512], P('dom'), may hold values from 0 to 7, as said below
- noise: float32 [2, 512, 2, 256, 128], P(None, 'dom'), may hold values from -6 to 6
- accept: int32 [2, 512], P(None, 'dom'), may hold values 0 or 1
- observed: float32 [256, 256], replicated, may hold values from -6 to 6
Outputs:
- moved: float32 [512, 2, 256, 128], P('dom')
- misfit: float32 [2, 512], P(None, 'dom')
The draws below stay inside these ranges and needn't reach their ends.
Inputs may be any that keep to these rules, and one draw needn't show every extreme that they name: `offspring`: the counts sum to 512. Slot s, numbered by the counts' running sum, is filled by a particle at most 3 places from s, and in every draw some slot is filled from exactly 3 places away.
All inputs are finite; a program needn't handle non-finite values. No bound on the sum of `accept` on one device may be relied on, other than what follows from the above.
Results may differ from the reference program's by a relative error of at most 0.0001.
Values sent between devices are 32-bit elements; how exact they have to be, the bound alone decides.
No kernel may reach another device: no remote copies, remote signals or barrier semaphores. Data moves between devices by JAX's collectives and lax.ppermute only.
A program may use at most 64 MiB of HBM per device.

```python
import jax
import jax.numpy as jnp
from jax import lax

G = 256
HALF = 128
MOVES = 2
STEPS = 1
LOW = 16
PARTICLES = 512
REACH = 3


def draw_particles(key, part):
    index_y = jnp.arange(G)
    wave_y = jnp.where(index_y < G // 2, index_y, index_y - G).astype(jnp.float32)
    wave_x = jnp.arange(G // 2).astype(jnp.float32)
    radius = jnp.sqrt(wave_y[:, None] ** 2 + wave_x[None, :] ** 2)
    spectrum = 1.5 / (1.0 + radius / 8.0)
    order = jnp.arange(PARTICLES).astype(jnp.float32) / max(PARTICLES - 1, 1)
    values = jax.random.normal(key, (PARTICLES, 2, G, G // 2), jnp.float32)
    rising = 1.0 + 2.0 * order
    return values * spectrum[None, None] * rising[:, None, None, None]


def draw_offspring(key, part):
    jumps = 4 * (jax.random.randint(jax.random.fold_in(key, 7), (PARTICLES,), 0, 4) == 0).astype(jnp.int32)
    walker = jnp.cumsum(jumps).astype(jnp.int32) - 2
    slot_ids = jnp.arange(PARTICLES, dtype=jnp.int32)
    base = jnp.clip(jnp.clip(walker, slot_ids - REACH, slot_ids + REACH), 0, PARTICLES - 1)
    center = jax.random.randint(jax.random.fold_in(key, 11), (), REACH, PARTICLES - REACH).astype(jnp.int32)
    source = jnp.where(jnp.abs(slot_ids - center) <= REACH, center, base).astype(jnp.int32)
    return jnp.zeros((PARTICLES,), jnp.int32).at[source].add(1)


def touch_ends(entries, own_key, low, high):
    shape = entries.shape
    spot = [jax.random.randint(jax.random.fold_in(own_key, axis), (), 0, shape[axis]) for axis in range(len(shape))]
    entries = entries.at[tuple(spot)].set(low)
    longest = shape.index(max(shape))
    spot[longest] = (spot[longest] + 1) % shape[longest]
    return entries.at[tuple(spot)].set(high)


def level_of(own_key, shape, cuts, smallest, largest):
    gain = 1.0
    for axis_at, shards_of in cuts:
        steps = jax.random.uniform(jax.random.fold_in(jax.random.fold_in(own_key, 6), axis_at), (shards_of,), jnp.float32, smallest / len(cuts), largest / len(cuts))
        gain = gain * jnp.repeat(jnp.exp(steps), shape[axis_at] // shards_of).reshape((-1,) + (1,) * (len(shape) - 1 - axis_at))
    return gain


def scatter_about(key, dims, scale, bound, pieces=(), held_as=jnp.bfloat16):
    result = scale * jax.random.normal(key, dims, jnp.float32)
    if pieces:
        result = result * level_of(key, dims, pieces, -0.22, 0.18)
    return jnp.clip(result, -bound, bound).astype(held_as)


def setup_inputs(seed: int = 0) -> dict:
    seeds = jax.random.split(jax.random.key(seed), 6)
    particles = draw_particles(jax.random.fold_in(seeds[5], 71), 0)
    offspring = draw_offspring(jax.random.fold_in(seeds[5], 71), 0)
    noise = scatter_about(seeds[2], (MOVES, PARTICLES, 2, G, HALF), 1.0, 6.0, ((1, 512),), jnp.float32)
    accept = touch_ends((jax.random.randint(seeds[3], (MOVES, PARTICLES), 0, 2) < 1).astype(jnp.int32), jax.random.fold_in(seeds[3], 1), 0, 1)
    observed = scatter_about(seeds[4], (G, G), 1.0, 6.0, (), jnp.float32)
    return dict(particles=particles, offspring=offspring, noise=noise, accept=accept, observed=observed)


time_step = 0.05
viscosity = 0.001
noise_level = 0.5
spectral_scale = 64.0
prior_amplitude = 1.5
step_size = 0.4

def wavenumbers():
    index_y = jnp.arange(G)
    wave_y = jnp.where(index_y < G // 2, index_y, index_y - G).astype(jnp.float32)
    wave_x = jnp.arange(G // 2).astype(jnp.float32)
    return (wave_y[:, None], wave_x[None, :])

def synthesize(coeffs):
    padded = jnp.pad(coeffs, ((0, 0), (0, 1)))
    return jnp.fft.irfft2(padded, s=(G, G)) * (G * G / spectral_scale)

def analyse(field):
    return jnp.fft.rfft2(field)[:, :G // 2] * (spectral_scale / (G * G))

def predicted_state(present_state, observed):
    wave_y, wave_x = wavenumbers()
    wave_sq = wave_y * wave_y + wave_x * wave_x
    inverse_sq = jnp.where(wave_sq > 0, 1.0 / jnp.maximum(wave_sq, 1.0), 0.0)
    keeper = ((jnp.abs(wave_y) <= G // 3) & (wave_x <= G // 3)).astype(jnp.float32)
    coeffs = lax.complex(present_state[0], present_state[1])
    for substep in range(STEPS):
        vort = synthesize(coeffs)
        stream = coeffs * inverse_sq
        vel_u = synthesize(1j * wave_y * stream)
        vel_v = synthesize(-1j * wave_x * stream)
        flux_u = analyse(vel_u * vort)
        flux_v = analyse(vel_v * vort)
        nonlin = (1j * wave_x * flux_u + 1j * wave_y * flux_v) * keeper
        coeffs = (coeffs - time_step * nonlin) / (1.0 + time_step * viscosity * wave_sq)
    final = synthesize(coeffs)
    return jnp.sum((final - observed) ** 2) / (2.0 * noise_level * noise_level * G * G)

def low_modes(block):
    return jnp.concatenate([block[..., :LOW // 2, :LOW], block[..., G - LOW // 2:, :LOW]], axis=-2)

def reference(particles, offspring, noise, accept, observed):
    ends = jnp.cumsum(offspring).astype(jnp.int32)
    slot_ids = jnp.arange(PARTICLES, dtype=jnp.int32)
    source = jnp.searchsorted(ends, slot_ids, side='right').astype(jnp.int32)
    present_state = jnp.take(particles, source, axis=0)
    power = lax.optimization_barrier(jnp.sum(low_modes(present_state) ** 2, axis=0)) / PARTICLES
    adapted = jnp.sqrt(power + 1e-06)
    wave_y, wave_x = wavenumbers()
    prior = prior_amplitude / (1.0 + jnp.sqrt(wave_y * wave_y + wave_x * wave_x) / 8.0)
    spread = jnp.stack([prior, prior]).astype(jnp.float32)
    spread = spread.at[:, :LOW // 2, :LOW].set(adapted[:, :LOW // 2])
    spread = spread.at[:, G - LOW // 2:, :LOW].set(adapted[:, LOW // 2:])
    keep = jnp.sqrt(1.0 - step_size * step_size)
    score_values = []
    for move in range(MOVES):
        candidate_state = keep * present_state + step_size * spread[None] * noise[move]
        score_values.append(lax.map(lambda lone_particle: predicted_state(lone_particle, observed), candidate_state))
        present_state = jnp.where(accept[move][:, None, None, None] == 1, candidate_state, present_state)
    return (present_state, jnp.stack(score_values).astype(jnp.float32))
```

```python
import functools
import math

import jax
import jax.numpy as jnp
import numpy as np
from jax import lax
from jax.experimental import pallas as pl
from jax.experimental.pallas import tpu as pltpu
from jax.sharding import PartitionSpec as P

MOVES = 2
LOW = 16
GRID = 256
HALF = 128
CUT = GRID // 3
BAND = 96
RING = 16
PLANE = 32
COUNTS = 64

time_step = 0.05
viscosity = 0.001
noise_level = 0.5
prior_amplitude = 1.5
step_size = 0.4
keep = math.sqrt(1.0 - step_size * step_size)

f32 = jnp.float32
bf16 = jnp.bfloat16


def split_table(table):
    high = table.astype(bf16)
    low = (table - high.astype(np.float64)).astype(bf16)
    return high, low


@functools.lru_cache(maxsize=1)
def tables():
    index = np.arange(GRID)
    phase = (index[:, None] * index[None, :] % GRID) * (2.0 * np.pi / GRID)
    cos, sin = np.cos(phase), np.sin(phase)
    across = np.concatenate([cos, sin], axis=1)
    down = np.concatenate([cos[:HALF], sin[:HALF]], axis=0)
    back = np.concatenate([cos[:, :HALF], sin[:, :HALF]], axis=1)
    parts = split_table(across) + split_table(down) + split_table(back)
    return np.concatenate(parts, axis=1)


def lanes(shape):
    return lax.broadcasted_iota(jnp.int32, shape, len(shape) - 1)


def first_kernel(ring_at, offspring_ref, top_ref, bottom_ref, tile_ref):
    count = offspring_ref[0].astype(f32)
    lane = lanes((8, 128))
    tile = jnp.where(lane == COUNTS + ring_at(), count, 0.0)
    for part in range(2):
        for side, ref in enumerate((top_ref, bottom_ref)):
            low = jnp.where(lane < LOW, ref[0, part], 0.0)
            square = count * (low * low)
            shift = (2 * part + side) * LOW
            tile += pltpu.roll(square, shift, 1) if shift else square
    tile_ref[...] = jnp.broadcast_to(tile[None], tile_ref.shape)


def second_kernel(tiles_ref, tile_ref):
    total = tiles_ref[0]
    for at in range(1, RING):
        total += tiles_ref[at]
    tile_ref[...] = jnp.broadcast_to(total[None], tile_ref.shape)


def split(value):
    high = value.astype(bf16)
    return high, (value - high.astype(f32)).astype(bf16)


def product(left_high, left_low, right_high, right_low):
    dot = functools.partial(jnp.dot, preferred_element_type=f32)
    return (
        dot(left_high, right_high) + dot(left_low, right_high) + dot(left_high, right_low)
    )


def final_kernel(
    slot_at,
    accept_ref,
    tiles_ref,
    own_ref,
    behind_ref,
    ahead_ref,
    partner_ref,
    far_ref,
    partner_behind_ref,
    partner_ahead_ref,
    noise_ref,
    observed_ref,
    table_ref,
    moved_ref,
    misfit_ref,
    chosen,
    moved_buf,
    data_high,
    data_low,
    in_sem,
    out_sem,
):
    across_high, across_low, down_high, down_low, back_high, back_low = (
        table_ref.at[:, start : start + size]
        for start, size in ((0, 512), (512, 512), (1024, 256), (1280, 256), (1536, 256), (1792, 256))
    )
    slot = slot_at()
    odd = lax.rem(slot, 2)

    counts = tiles_ref[:, 0, :]
    lane = lanes((PLANE, 128))
    plane_at = lax.broadcasted_iota(jnp.int32, (PLANE, 128), 0)
    place = (lane - COUNTS) * PLANE + plane_at
    counted = (lane >= COUNTS) & (lane < COUNTS + RING)
    offset = jnp.full((1, 1), -3, jnp.int32)
    for distance in range(-3, 4):
        ends = jnp.sum(
            jnp.where(counted & (place <= slot + distance), counts, 0.0), keepdims=True
        )
        offset += (ends <= slot.astype(f32)).astype(jnp.int32)
    offset = jnp.minimum(offset, 3)[0, 0]

    side = 1 - 2 * odd
    candidates = (
        (0, own_ref),
        (-2, behind_ref),
        (2, ahead_ref),
        (side, partner_ref),
        (-3 * side, far_ref),
        (side - 2, partner_behind_ref),
        (side + 2, partner_ahead_ref),
    )
    for at, ref in candidates:

        @pl.when(offset == at)
        def _(ref=ref):
            pltpu.make_async_copy(ref.at[0], chosen, in_sem).start()

    row = lax.broadcasted_iota(jnp.int32, (GRID, HALF), 0)
    wave_x = lanes((GRID, HALF)).astype(f32)
    wave_y = jnp.where(row < GRID // 2, row, row - GRID).astype(f32)
    wave_sq = wave_y * wave_y + wave_x * wave_x
    inverse_sq = jnp.where(wave_sq > 0, 1.0 / jnp.maximum(wave_sq, 1.0), 0.0)
    along = wave_y * inverse_sq
    cross = wave_x * inverse_sq
    weight = jnp.where(lanes((GRID, HALF)) == 0, 1.0 / 64, 2.0 / 64)
    prior = prior_amplitude / (1.0 + jnp.sqrt(wave_sq) / 8.0)
    decay = 1.0 / (1.0 + time_step * viscosity * wave_sq)
    keeper = ((jnp.abs(wave_y) <= CUT) & (wave_x <= CUT)).astype(f32)
    pull = keeper * (time_step * 64.0 / (GRID * GRID))

    total = tiles_ref[0]
    for at in range(1, PLANE):
        total += tiles_ref[at]
    adapted = jnp.sqrt(jnp.maximum(total, 0.0) / (RING * PLANE) + 1e-06)
    low_lane = lanes((8, HALF)) < LOW

    def spread(part):
        top, bottom = adapted, pltpu.roll(adapted, 128 - LOW, 1)
        if part:
            top = pltpu.roll(adapted, 128 - 2 * LOW, 1)
            bottom = pltpu.roll(adapted, 128 - 3 * LOW, 1)
        return jnp.concatenate(
            [
                jnp.where(low_lane, top, prior[:8]),
                prior[8 : GRID - 8],
                jnp.where(low_lane, bottom, prior[GRID - 8 :]),
            ],
            axis=0,
        )

    scale = [step_size * spread(part) for part in range(2)]

    pltpu.make_async_copy(own_ref.at[0], chosen, in_sem).wait()
    current = [chosen[part] for part in range(2)]
    proposals = []
    for move in range(MOVES):
        proposal = [keep * current[part] + scale[part] * noise_ref[move, 0, part] for part in range(2)]
        proposals.append(proposal)
        taken = accept_ref[move] == 1
        current = [jnp.where(taken, proposal[part], current[part]) for part in range(2)]
    for part in range(2):
        moved_buf[part] = current[part]
    out_copy = pltpu.make_async_copy(moved_buf, moved_ref.at[0], out_sem)
    out_copy.start()

    def load(slot_in, real, imag):
        real_high, real_low = split(real)
        imag_high, imag_low = split(imag)
        for ref, re, im in ((data_high, real_high, imag_high), (data_low, real_low, imag_low)):
            ref[slot_in, :GRID, :HALF] = re
            ref[slot_in, :GRID, HALF:] = -im
            ref[slot_in, GRID:, :HALF] = -im
            ref[slot_in, GRID:, HALF:] = -re

    def synthesize(slot_in, real, imag):
        load(slot_in, real, imag)
        rows = product(across_high[...], across_low[...], data_high[slot_in], data_low[slot_in])
        return product(*split(rows), down_high[...], down_low[...])

    def analyse(slot_in, field):
        rows = product(*split(field), back_high[...], back_low[...])
        load(slot_in, rows[:, :HALF], rows[:, HALF:])
        return [
            product(
                across_high[start : start + BAND],
                across_low[start : start + BAND],
                data_high[slot_in],
                data_low[slot_in],
            )
            for start in (0, GRID - BAND)
        ]

    scores = jnp.zeros((1, MOVES), f32)
    for move in range(MOVES):
        real, imag = proposals[move]
        base = 3 * move
        wr, wi = real * weight, imag * weight
        vort = synthesize(base, wr, wi)
        flow_u = synthesize(base + 1, -along * wi, along * wr)
        flow_v = synthesize(base + 2, cross * wi, -cross * wr)
        flux_u = analyse(base, flow_u * vort)
        flux_v = analyse(base + 1, flow_v * vort)
        push_re, push_im = [], []
        for at, start in enumerate((0, GRID - BAND)):
            kx, ky = (w[start : start + BAND] for w in (wave_x, wave_y))
            factor = pull[start : start + BAND]
            push_re.append(
                factor * (kx * flux_u[at][:, HALF:] + ky * flux_v[at][:, HALF:])
            )
            push_im.append(
                -factor * (kx * flux_u[at][:, :HALF] + ky * flux_v[at][:, :HALF])
            )
        middle = jnp.zeros((GRID - 2 * BAND, HALF), f32)
        change_re = jnp.concatenate([push_re[0], middle, push_re[1]], axis=0)
        change_im = jnp.concatenate([push_im[0], middle, push_im[1]], axis=0)
        final = synthesize(
            base + 2,
            (real + change_re) * decay * weight,
            (imag + change_im) * decay * weight,
        )
        gap = final - observed_ref[...]
        score = jnp.sum(gap * gap, keepdims=True) * (
            1.0 / (2.0 * noise_level * noise_level * GRID * GRID)
        )
        scores = jnp.where(lanes((1, MOVES)) == move, score, scores)
    misfit_ref[...] = scores
    out_copy.wait()


def whole(*shape):
    return pl.BlockSpec(memory_space=pltpu.VMEM)


def body(particles, offspring, noise, accept, observed):
    devices = RING * PLANE
    rings = [[z * PLANE + at for z in range(RING)] for at in range(PLANE)]
    planes = [[z * PLANE + at for at in range(PLANE)] for z in range(RING)]
    vmem, smem = pl.BlockSpec(memory_space=pltpu.VMEM), pl.BlockSpec(memory_space=pltpu.SMEM)
    anywhere = pl.BlockSpec(memory_space=pl.ANY)

    def gather(tiles, groups):
        return lax.all_to_all(tiles, "dom", 0, 0, axis_index_groups=groups, tiled=True)

    def send(value, target):
        pairs = [(i, target(i)) for i in range(devices) if 0 <= target(i) < devices]
        return lax.ppermute(value, "dom", pairs)

    slot_at = lambda: lax.axis_index("dom")
    tile = pl.pallas_call(
        functools.partial(first_kernel, lambda: lax.div(slot_at(), PLANE)),
        grid=(1,),
        in_specs=[
            smem,
            pl.BlockSpec((1, 2, 8, HALF), lambda i: (0, 0, 0, 0)),
            pl.BlockSpec((1, 2, 8, HALF), lambda i: (0, 0, GRID // 8 - 1, 0)),
        ],
        out_specs=pl.BlockSpec((RING, 8, 128), lambda i: (0, 0, 0)),
        out_shape=jax.ShapeDtypeStruct((RING, 8, 128), f32),
        compiler_params=pltpu.CompilerParams(vmem_limit_bytes=2 * 1024 * 1024),
        name="first",
    )(offspring, particles, particles)
    behind = send(particles, lambda i: i + 2)
    ahead = send(particles, lambda i: i - 2)
    partner = send(particles, lambda i: i ^ 1)
    far = send(particles, lambda i: i + 3 if i % 2 else i - 3)
    ring = gather(tile, rings)
    tile = pl.pallas_call(
        second_kernel,
        in_specs=[vmem],
        out_specs=vmem,
        out_shape=jax.ShapeDtypeStruct((PLANE, 8, 128), f32),
        compiler_params=pltpu.CompilerParams(vmem_limit_bytes=2 * 1024 * 1024),
        name="second",
    )(ring)
    partner_behind = send(behind, lambda i: i ^ 1)
    partner_ahead = send(ahead, lambda i: i ^ 1)
    tiles = gather(tile, planes)
    moved, misfit = pl.pallas_call(
        functools.partial(final_kernel, slot_at),
        in_specs=[smem, vmem] + [anywhere] * 7 + [vmem] * 3,
        out_specs=[anywhere, vmem],
        out_shape=[
            jax.ShapeDtypeStruct((1, 2, GRID, HALF), f32),
            jax.ShapeDtypeStruct((1, MOVES), f32),
        ],
        scratch_shapes=[
            pltpu.VMEM((2, GRID, HALF), f32),
            pltpu.VMEM((2, GRID, HALF), f32),
            pltpu.VMEM((6, 2 * GRID, GRID), bf16),
            pltpu.VMEM((6, 2 * GRID, GRID), bf16),
            pltpu.SemaphoreType.DMA,
            pltpu.SemaphoreType.DMA,
        ],
        compiler_params=pltpu.CompilerParams(vmem_limit_bytes=24 * 1024 * 1024),
        name="final",
    )(
        accept.reshape(MOVES),
        tiles,
        particles,
        behind,
        ahead,
        partner,
        far,
        partner_behind,
        partner_ahead,
        noise,
        observed,
        jnp.asarray(tables()),
    )
    return moved, misfit.reshape(MOVES, 1)


def solution(mesh):
    return jax.shard_map(
        body,
        mesh=mesh,
        in_specs=(
            P("dom", None, None, None),
            P("dom"),
            P(None, "dom", None, None, None),
            P(None, "dom"),
            P(),
        ),
        out_specs=(P("dom", None, None, None), P(None, "dom")),
        check_vma=False,
    )
```

```python
import functools
import math

import jax
import jax.numpy as jnp
import numpy as np
from jax import lax
from jax.experimental import pallas as pl
from jax.experimental.pallas import tpu as pltpu
from jax.sharding import PartitionSpec as P

MOVES = 2
LOW = 16
GRID = 256
HALF = 128
CUT = GRID // 3
BAND = 96
RING = 16
PLANE = 32
COUNTS = 64

time_step = 0.05
viscosity = 0.001
noise_level = 0.5
prior_amplitude = 1.5
step_size = 0.4
keep = math.sqrt(1.0 - step_size * step_size)

f32 = jnp.float32
bf16 = jnp.bfloat16


def split_table(table):
    high = table.astype(bf16)
    low = (table - high.astype(np.float64)).astype(bf16)
    return high, low


@functools.lru_cache(maxsize=1)
def tables():
    index = np.arange(GRID)
    phase = (index[:, None] * index[None, :] % GRID) * (2.0 * np.pi / GRID)
    cos, sin = np.cos(phase), np.sin(phase)
    turned = sin[:HALF].copy()
    turned[0] = 1.0 - 2.0 * (index % 2)
    across = np.concatenate([cos[:HALF], turned], axis=0)
    down = np.concatenate([cos[:HALF], -sin[:HALF]], axis=0)
    back = np.concatenate([cos[:, :HALF], sin[:, :HALF]], axis=1)
    parts = [half for t in (across, down, back, across.T) for half in split_table(t)]
    return np.concatenate(parts, axis=1)


def lanes(shape):
    return lax.broadcasted_iota(jnp.int32, shape, len(shape) - 1)


def first_kernel(plane_at, offspring_ref, top_ref, bottom_ref, tile_ref):
    count = offspring_ref[0].astype(f32)
    lane = lanes((8, 128))
    tile = jnp.where(lane == COUNTS + plane_at(), count, 0.0)
    for part in range(2):
        for side, ref in enumerate((top_ref, bottom_ref)):
            low = jnp.where(lane < LOW, ref[0, part], 0.0)
            square = count * (low * low)
            shift = (2 * part + side) * LOW
            tile += pltpu.roll(square, shift, 1) if shift else square
    tile_ref[...] = jnp.broadcast_to(tile[None], tile_ref.shape)


def second_kernel(tiles_ref, tile_ref):
    total = tiles_ref[0]
    for at in range(1, PLANE):
        total += tiles_ref[at]
    tile_ref[...] = jnp.broadcast_to(total[None], tile_ref.shape)


def split(value):
    high = value.astype(bf16)
    return high, (value - high.astype(f32)).astype(bf16)


def backwards(rows):
    count, width = rows.shape
    groups = pltpu.roll(rows, count - 1, 0).reshape(count // 8, 8, width)
    sub = lax.broadcasted_iota(jnp.int32, groups.shape, 1)
    for step in (4, 2, 1):
        up, lower = pltpu.roll(groups, 8 - step, 1), pltpu.roll(groups, step, 1)
        groups = jnp.where(lax.rem(lax.div(sub, step), 2) == 0, up, lower)
    return jnp.concatenate([groups[i] for i in range(count // 8)][::-1], axis=0)


def product(left_high, left_low, right_high, right_low):
    dot = functools.partial(jnp.dot, preferred_element_type=f32)
    return (
        dot(left_high, right_high) + dot(left_low, right_high) + dot(left_high, right_low)
    )


def final_kernel(
    slot_at,
    accept_ref,
    tiles_ref,
    own_ref,
    behind_ref,
    ahead_ref,
    partner_ref,
    far_ref,
    partner_behind_ref,
    partner_ahead_ref,
    noise_ref,
    observed_ref,
    table_ref,
    moved_ref,
    misfit_ref,
    chosen,
    moved_buf,
    data_high,
    data_low,
    table_buf,
    table_sem,
    in_sem,
    out_sem,
):
    table_copy = pltpu.make_async_copy(table_ref, table_buf, table_sem)
    table_copy.start()
    across, down, back, gather = (
        [table_buf.at[:, start : start + GRID] for start in (at, at + GRID)]
        for at in range(0, 8 * GRID, 2 * GRID)
    )
    slot = slot_at()
    odd = lax.rem(slot, 2)

    counts = tiles_ref[:, 0, :]
    lane = lanes((RING, 128))
    ring_at = lax.broadcasted_iota(jnp.int32, (RING, 128), 0)
    place = ring_at * PLANE + lane - COUNTS
    counted = (lane >= COUNTS) & (lane < COUNTS + PLANE)
    offset = jnp.full((1, 1), -3, jnp.int32)
    for distance in range(-3, 4):
        ends = jnp.sum(
            jnp.where(counted & (place <= slot + distance), counts, 0.0), keepdims=True
        )
        offset += (ends <= slot.astype(f32)).astype(jnp.int32)
    offset = jnp.minimum(offset, 3)[0, 0]

    side = 1 - 2 * odd
    candidates = (
        (0, own_ref),
        (-2, behind_ref),
        (2, ahead_ref),
        (side, partner_ref),
        (-3 * side, far_ref),
        (side - 2, partner_behind_ref),
        (side + 2, partner_ahead_ref),
    )
    for at, ref in candidates:

        @pl.when(offset == at)
        def _(ref=ref):
            pltpu.make_async_copy(ref.at[0], chosen, in_sem).start()

    row = lax.broadcasted_iota(jnp.int32, (GRID, HALF), 0)
    wave_x = lanes((GRID, HALF)).astype(f32)
    wave_y = jnp.where(row < GRID // 2, row, row - GRID).astype(f32)
    wave_sq = wave_y * wave_y + wave_x * wave_x
    inverse_sq = jnp.where(wave_sq > 0, 1.0 / jnp.maximum(wave_sq, 1.0), 0.0)
    along = wave_y * inverse_sq
    cross = wave_x * inverse_sq
    weight = jnp.where(lanes((GRID, HALF)) == 0, 1.0 / 64, 2.0 / 64)
    prior = prior_amplitude / (1.0 + jnp.sqrt(wave_sq) / 8.0)
    decay = 1.0 / (1.0 + time_step * viscosity * wave_sq)
    keeper = ((jnp.abs(wave_y) <= CUT) & (wave_x <= CUT)).astype(f32)
    pull = keeper * (time_step * 64.0 / (GRID * GRID))

    total = tiles_ref[0]
    for at in range(1, RING):
        total += tiles_ref[at]
    adapted = jnp.sqrt(jnp.maximum(total, 0.0) / (RING * PLANE) + 1e-06)
    low_lane = lanes((8, HALF)) < LOW

    def spread(part):
        top, bottom = adapted, pltpu.roll(adapted, 128 - LOW, 1)
        if part:
            top = pltpu.roll(adapted, 128 - 2 * LOW, 1)
            bottom = pltpu.roll(adapted, 128 - 3 * LOW, 1)
        return jnp.concatenate(
            [
                jnp.where(low_lane, top, prior[:8]),
                prior[8 : GRID - 8],
                jnp.where(low_lane, bottom, prior[GRID - 8 :]),
            ],
            axis=0,
        )

    scale = [step_size * spread(part) for part in range(2)]

    pltpu.make_async_copy(own_ref.at[0], chosen, in_sem).wait()
    current = [chosen[part] for part in range(2)]
    proposals = []
    for move in range(MOVES):
        proposal = [keep * current[part] + scale[part] * noise_ref[move, 0, part] for part in range(2)]
        proposals.append(proposal)
        taken = accept_ref[move] == 1
        current = [jnp.where(taken, proposal[part], current[part]) for part in range(2)]
    for part in range(2):
        moved_buf[part] = current[part]
    out_copy = pltpu.make_async_copy(moved_buf, moved_ref.at[0], out_sem)
    out_copy.start()

    table_copy.wait()

    def synthesize(at, real, imag):
        for half, value in enumerate((real, imag)):
            high, low = split(value)
            data_high[at, :, half * HALF : (half + 1) * HALF] = high
            data_low[at, :, half * HALF : (half + 1) * HALF] = low
        both = product(across[0][...], across[1][...], data_high[at], data_low[at])
        even_re, even_im = both[:HALF, :HALF], both[:HALF, HALF:]
        odd_re, odd_im = both[HALF:, :HALF], both[HALF:, HALF:]
        rows_re = jnp.concatenate(
            [
                jnp.where(first_row, even_re, even_re - odd_im),
                jnp.where(first_row, odd_re, even_re + odd_im),
            ],
            axis=0,
        )
        rows_im = jnp.concatenate(
            [
                jnp.where(first_row, even_im, even_im + odd_re),
                jnp.where(first_row, odd_im, even_im - odd_re),
            ],
            axis=0,
        )
        rows = jnp.concatenate([rows_re, rows_im], axis=1)
        return product(*split(rows), down[0][...], down[1][...])

    def analyse(at, field):
        rows = product(*split(field), back[0][...], back[1][...])
        plus_c, plus_s = rows[:HALF, :HALF], rows[:HALF, HALF:]
        minus_c, minus_s = rows[HALF:, :HALF], rows[HALF:, HALF:]
        quarters = (
            (0, 0, jnp.where(first_row, plus_c, plus_c + minus_c)),
            (0, HALF, -jnp.where(first_row, plus_s, plus_s + minus_s)),
            (HALF, 0, jnp.where(first_row, minus_c, minus_s - plus_s)),
            (HALF, HALF, jnp.where(first_row, -minus_s, minus_c - plus_c)),
        )
        for row, column, value in quarters:
            high, low = split(value)
            data_high[at, row : row + HALF, column : column + HALF] = high
            data_low[at, row : row + HALF, column : column + HALF] = low
        return [
            product(
                gather[0][start : start + BAND],
                gather[1][start : start + BAND],
                data_high[at],
                data_low[at],
            )
            for start in (0, GRID - BAND)
        ]

    first_row = lax.broadcasted_iota(jnp.int32, (HALF, HALF), 0) == 0
    target = jnp.concatenate(
        [observed_ref[:HALF], backwards(observed_ref[HALF:])], axis=0
    )

    scores = jnp.zeros((1, MOVES), f32)
    for move in range(MOVES):
        real, imag = proposals[move]
        base = 3 * move
        wr, wi = real * weight, imag * weight
        vort = synthesize(base, wr, wi)
        flow_u = synthesize(base + 1, -along * wi, along * wr)
        flow_v = synthesize(base + 2, cross * wi, -cross * wr)
        flux_u = analyse(base, flow_u * vort)
        flux_v = analyse(base + 1, flow_v * vort)
        push_re, push_im = [], []
        for at, start in enumerate((0, GRID - BAND)):
            kx, ky = (w[start : start + BAND] for w in (wave_x, wave_y))
            factor = pull[start : start + BAND]
            push_re.append(
                factor * (kx * flux_u[at][:, HALF:] + ky * flux_v[at][:, HALF:])
            )
            push_im.append(
                -factor * (kx * flux_u[at][:, :HALF] + ky * flux_v[at][:, :HALF])
            )
        middle = jnp.zeros((GRID - 2 * BAND, HALF), f32)
        change_re = jnp.concatenate([push_re[0], middle, push_re[1]], axis=0)
        change_im = jnp.concatenate([push_im[0], middle, push_im[1]], axis=0)
        final = synthesize(
            base + 2,
            (real + change_re) * decay * weight,
            (imag + change_im) * decay * weight,
        )
        gap = final - target
        score = jnp.sum(gap * gap, keepdims=True) * (
            1.0 / (2.0 * noise_level * noise_level * GRID * GRID)
        )
        scores = jnp.where(lanes((1, MOVES)) == move, score, scores)
    misfit_ref[...] = scores
    out_copy.wait()


def body(particles, offspring, noise, accept, observed):
    devices = RING * PLANE
    rings = [[z * PLANE + at for z in range(RING)] for at in range(PLANE)]
    planes = [[z * PLANE + at for at in range(PLANE)] for z in range(RING)]
    vmem, smem = pl.BlockSpec(memory_space=pltpu.VMEM), pl.BlockSpec(memory_space=pltpu.SMEM)
    anywhere = pl.BlockSpec(memory_space=pl.ANY)

    def gather(tiles, groups):
        return lax.all_to_all(tiles, "dom", 0, 0, axis_index_groups=groups, tiled=True)

    def send(value, target):
        pairs = [(i, target(i)) for i in range(devices) if 0 <= target(i) < devices]
        return lax.ppermute(value, "dom", pairs)

    slot_at = lambda: lax.axis_index("dom")
    tile = pl.pallas_call(
        functools.partial(first_kernel, lambda: lax.rem(slot_at(), PLANE)),
        grid=(1,),
        in_specs=[
            smem,
            pl.BlockSpec((1, 2, 8, HALF), lambda i: (0, 0, 0, 0)),
            pl.BlockSpec((1, 2, 8, HALF), lambda i: (0, 0, GRID // 8 - 1, 0)),
        ],
        out_specs=pl.BlockSpec((PLANE, 8, 128), lambda i: (0, 0, 0)),
        out_shape=jax.ShapeDtypeStruct((PLANE, 8, 128), f32),
        compiler_params=pltpu.CompilerParams(vmem_limit_bytes=2 * 1024 * 1024),
        name="first",
    )(offspring, particles, particles)
    behind = send(particles, lambda i: i + 2)
    ahead = send(particles, lambda i: i - 2)
    partner = send(particles, lambda i: i ^ 1)
    far = send(particles, lambda i: i + 3 if i % 2 else i - 3)
    plane = gather(tile, planes)
    tile = pl.pallas_call(
        second_kernel,
        in_specs=[vmem],
        out_specs=vmem,
        out_shape=jax.ShapeDtypeStruct((RING, 8, 128), f32),
        compiler_params=pltpu.CompilerParams(vmem_limit_bytes=2 * 1024 * 1024),
        name="second",
    )(plane)
    partner_behind = send(behind, lambda i: i ^ 1)
    partner_ahead = send(ahead, lambda i: i ^ 1)
    tiles = gather(tile, rings)
    moved, misfit = pl.pallas_call(
        functools.partial(final_kernel, slot_at),
        in_specs=[smem, vmem] + [anywhere] * 7 + [vmem] * 2 + [anywhere],
        out_specs=[anywhere, vmem],
        out_shape=[
            jax.ShapeDtypeStruct((1, 2, GRID, HALF), f32),
            jax.ShapeDtypeStruct((1, MOVES), f32),
        ],
        scratch_shapes=[
            pltpu.VMEM((2, GRID, HALF), f32),
            pltpu.VMEM((2, GRID, HALF), f32),
            pltpu.VMEM((6, GRID, GRID), bf16),
            pltpu.VMEM((6, GRID, GRID), bf16),
            pltpu.VMEM((GRID, 8 * GRID), bf16),
            pltpu.SemaphoreType.DMA,
            pltpu.SemaphoreType.DMA,
            pltpu.SemaphoreType.DMA,
        ],
        compiler_params=pltpu.CompilerParams(vmem_limit_bytes=24 * 1024 * 1024),
        name="final",
    )(
        accept.reshape(MOVES),
        tiles,
        particles,
        behind,
        ahead,
        partner,
        far,
        partner_behind,
        partner_ahead,
        noise,
        observed,
        pltpu.with_memory_space_constraint(jnp.asarray(tables()), pltpu.HBM),
    )
    return moved, misfit.reshape(MOVES, 1)


def solution(mesh):
    return jax.shard_map(
        body,
        mesh=mesh,
        in_specs=(
            P("dom", None, None, None),
            P("dom"),
            P(None, "dom", None, None, None),
            P(None, "dom"),
            P(),
        ),
        out_specs=(P("dom", None, None, None), P(None, "dom")),
        check_vma=False,
    )
```

```python
import functools
import math

import jax
import jax.numpy as jnp
import numpy as np
from jax import lax
from jax.experimental import pallas as pl
from jax.experimental.pallas import tpu as pltpu
from jax.sharding import PartitionSpec as P

MOVES = 2
LOW = 16
GRID = 256
HALF = 128
CUT = GRID // 3
BAND = 96
RING = 16
PLANE = 32
COUNTS = 64

time_step = 0.05
viscosity = 0.001
noise_level = 0.5
prior_amplitude = 1.5
step_size = 0.4
keep = math.sqrt(1.0 - step_size * step_size)

f32 = jnp.float32
bf16 = jnp.bfloat16


def split_table(table):
    high = table.astype(bf16)
    low = (table - high.astype(np.float64)).astype(bf16)
    return high, low


@functools.lru_cache(maxsize=1)
def tables():
    index = np.arange(GRID)
    phase = (index[:, None] * index[None, :] % GRID) * (2.0 * np.pi / GRID)
    cos, sin = np.cos(phase), np.sin(phase)
    turned = sin[:HALF].copy()
    turned[0] = 1.0 - 2.0 * (index % 2)
    across = np.concatenate([cos[:HALF], turned], axis=0)
    down = np.concatenate([cos[:HALF], -sin[:HALF]], axis=0)
    back = np.concatenate([cos[:, :HALF], sin[:, :HALF]], axis=1)
    parts = [half for t in (across, down, back, across.T) for half in split_table(t)]
    return np.concatenate(parts, axis=1)


def lanes(shape):
    return lax.broadcasted_iota(jnp.int32, shape, len(shape) - 1)


def first_kernel(plane_at, offspring_ref, particle_ref, tile_ref, low_buf, sems):
    copies = [
        pltpu.make_async_copy(
            particle_ref.at[0, :, pl.ds(start, 8)], low_buf.at[side], sems.at[side]
        )
        for side, start in enumerate((0, GRID - 8))
    ]
    for copy in copies:
        copy.start()
    for copy in copies:
        copy.wait()
    count = offspring_ref[...]
    lane = lanes((8, 128))
    tile = jnp.where(lane == COUNTS + plane_at(), count, 0.0)
    for part in range(2):
        for side in range(2):
            low = jnp.where(lane < LOW, low_buf[side, part], 0.0)
            square = count * (low * low)
            shift = (2 * part + side) * LOW
            tile += pltpu.roll(square, shift, 1) if shift else square
    tile_ref[...] = jnp.broadcast_to(tile[None], tile_ref.shape)


def second_kernel(tiles_ref, tile_ref):
    total = tiles_ref[0]
    for at in range(1, PLANE):
        total += tiles_ref[at]
    tile_ref[...] = jnp.broadcast_to(total[None], tile_ref.shape)


def split(value):
    high = value.astype(bf16)
    return high, (value - high.astype(f32)).astype(bf16)


def backwards(rows):
    count, width = rows.shape
    groups = pltpu.roll(rows, count - 1, 0).reshape(count // 8, 8, width)
    sub = lax.broadcasted_iota(jnp.int32, groups.shape, 1)
    for step in (4, 2, 1):
        up, lower = pltpu.roll(groups, 8 - step, 1), pltpu.roll(groups, step, 1)
        groups = jnp.where(lax.rem(lax.div(sub, step), 2) == 0, up, lower)
    return jnp.concatenate([groups[i] for i in range(count // 8)][::-1], axis=0)


def product(left_high, left_low, right_high, right_low):
    dot = functools.partial(jnp.dot, preferred_element_type=f32)
    return (
        dot(left_high, right_high) + dot(left_low, right_high) + dot(left_high, right_low)
    )


def final_kernel(
    slot_at,
    accept_ref,
    tiles_ref,
    own_ref,
    behind_ref,
    ahead_ref,
    partner_ref,
    far_ref,
    partner_behind_ref,
    partner_ahead_ref,
    noise_ref,
    observed_ref,
    table_ref,
    moved_ref,
    misfit_ref,
    chosen,
    moved_buf,
    data_high,
    data_low,
    table_buf,
    observed_buf,
    table_sem,
    observed_sem,
    in_sem,
    out_sem,
):
    table_copy = pltpu.make_async_copy(table_ref, table_buf, table_sem)
    table_copy.start()
    observed_copy = pltpu.make_async_copy(observed_ref, observed_buf, observed_sem)
    observed_copy.start()
    across, down, back, gather = (
        [table_buf.at[:, start : start + GRID] for start in (at, at + GRID)]
        for at in range(0, 8 * GRID, 2 * GRID)
    )
    slot = slot_at()
    odd = lax.rem(slot, 2)

    counts = tiles_ref[:, 0, :]
    lane = lanes((RING, 128))
    ring_at = lax.broadcasted_iota(jnp.int32, (RING, 128), 0)
    place = ring_at * PLANE + lane - COUNTS
    counted = (lane >= COUNTS) & (lane < COUNTS + PLANE)
    offset = jnp.full((1, 1), -3, jnp.int32)
    for distance in range(-3, 4):
        ends = jnp.sum(
            jnp.where(counted & (place <= slot + distance), counts, 0.0), keepdims=True
        )
        offset += (ends <= slot.astype(f32)).astype(jnp.int32)
    offset = jnp.minimum(offset, 3)[0, 0]

    side = 1 - 2 * odd
    candidates = (
        (0, own_ref),
        (-2, behind_ref),
        (2, ahead_ref),
        (side, partner_ref),
        (-3 * side, far_ref),
        (side - 2, partner_behind_ref),
        (side + 2, partner_ahead_ref),
    )
    for at, ref in candidates:

        @pl.when(offset == at)
        def _(ref=ref):
            pltpu.make_async_copy(ref.at[0], chosen, in_sem).start()

    row = lax.broadcasted_iota(jnp.int32, (GRID, HALF), 0)
    wave_x = lanes((GRID, HALF)).astype(f32)
    wave_y = jnp.where(row < GRID // 2, row, row - GRID).astype(f32)
    wave_sq = wave_y * wave_y + wave_x * wave_x
    inverse_sq = jnp.where(wave_sq > 0, 1.0 / jnp.maximum(wave_sq, 1.0), 0.0)
    along = wave_y * inverse_sq
    cross = wave_x * inverse_sq
    weight = jnp.where(lanes((GRID, HALF)) == 0, 1.0 / 64, 2.0 / 64)
    prior = prior_amplitude / (1.0 + jnp.sqrt(wave_sq) / 8.0)
    decay = 1.0 / (1.0 + time_step * viscosity * wave_sq)
    keeper = ((jnp.abs(wave_y) <= CUT) & (wave_x <= CUT)).astype(f32)
    pull = keeper * (time_step * 64.0 / (GRID * GRID))

    total = tiles_ref[0]
    for at in range(1, RING):
        total += tiles_ref[at]
    adapted = jnp.sqrt(jnp.maximum(total, 0.0) / (RING * PLANE) + 1e-06)
    low_lane = lanes((8, HALF)) < LOW

    def spread(part):
        top, bottom = adapted, pltpu.roll(adapted, 128 - LOW, 1)
        if part:
            top = pltpu.roll(adapted, 128 - 2 * LOW, 1)
            bottom = pltpu.roll(adapted, 128 - 3 * LOW, 1)
        return jnp.concatenate(
            [
                jnp.where(low_lane, top, prior[:8]),
                prior[8 : GRID - 8],
                jnp.where(low_lane, bottom, prior[GRID - 8 :]),
            ],
            axis=0,
        )

    scale = [step_size * spread(part) for part in range(2)]

    pltpu.make_async_copy(own_ref.at[0], chosen, in_sem).wait()
    current = [chosen[part] for part in range(2)]
    proposals = []
    for move in range(MOVES):
        proposal = [keep * current[part] + scale[part] * noise_ref[move, 0, part] for part in range(2)]
        proposals.append(proposal)
        taken = accept_ref[move] == 1
        current = [jnp.where(taken, proposal[part], current[part]) for part in range(2)]
    for part in range(2):
        moved_buf[part] = current[part]
    out_copy = pltpu.make_async_copy(moved_buf, moved_ref.at[0], out_sem)
    out_copy.start()

    table_copy.wait()
    observed_copy.wait()

    def synthesize(at, real, imag):
        for half, value in enumerate((real, imag)):
            high, low = split(value)
            data_high[at, :, half * HALF : (half + 1) * HALF] = high
            data_low[at, :, half * HALF : (half + 1) * HALF] = low
        both = product(across[0][...], across[1][...], data_high[at], data_low[at])
        even_re, even_im = both[:HALF, :HALF], both[:HALF, HALF:]
        odd_re, odd_im = both[HALF:, :HALF], both[HALF:, HALF:]
        rows_re = jnp.concatenate(
            [
                jnp.where(first_row, even_re, even_re - odd_im),
                jnp.where(first_row, odd_re, even_re + odd_im),
            ],
            axis=0,
        )
        rows_im = jnp.concatenate(
            [
                jnp.where(first_row, even_im, even_im + odd_re),
                jnp.where(first_row, odd_im, even_im - odd_re),
            ],
            axis=0,
        )
        rows = jnp.concatenate([rows_re, rows_im], axis=1)
        return product(*split(rows), down[0][...], down[1][...])

    def analyse(at, field):
        rows = product(*split(field), back[0][...], back[1][...])
        plus_c, plus_s = rows[:HALF, :HALF], rows[:HALF, HALF:]
        minus_c, minus_s = rows[HALF:, :HALF], rows[HALF:, HALF:]
        quarters = (
            (0, 0, jnp.where(first_row, plus_c, plus_c + minus_c)),
            (0, HALF, -jnp.where(first_row, plus_s, plus_s + minus_s)),
            (HALF, 0, jnp.where(first_row, minus_c, minus_s - plus_s)),
            (HALF, HALF, jnp.where(first_row, -minus_s, minus_c - plus_c)),
        )
        for row, column, value in quarters:
            high, low = split(value)
            data_high[at, row : row + HALF, column : column + HALF] = high
            data_low[at, row : row + HALF, column : column + HALF] = low
        return [
            product(
                gather[0][start : start + BAND],
                gather[1][start : start + BAND],
                data_high[at],
                data_low[at],
            )
            for start in (0, GRID - BAND)
        ]

    first_row = lax.broadcasted_iota(jnp.int32, (HALF, HALF), 0) == 0
    target = jnp.concatenate(
        [observed_buf[:HALF], backwards(observed_buf[HALF:])], axis=0
    )

    scores = jnp.zeros((1, MOVES), f32)
    for move in range(MOVES):
        real, imag = proposals[move]
        base = 3 * move
        wr, wi = real * weight, imag * weight
        vort = synthesize(base, wr, wi)
        flow_u = synthesize(base + 1, -along * wi, along * wr)
        flow_v = synthesize(base + 2, cross * wi, -cross * wr)
        flux_u = analyse(base, flow_u * vort)
        flux_v = analyse(base + 1, flow_v * vort)
        push_re, push_im = [], []
        for at, start in enumerate((0, GRID - BAND)):
            kx, ky = (w[start : start + BAND] for w in (wave_x, wave_y))
            factor = pull[start : start + BAND]
            push_re.append(
                factor * (kx * flux_u[at][:, HALF:] + ky * flux_v[at][:, HALF:])
            )
            push_im.append(
                -factor * (kx * flux_u[at][:, :HALF] + ky * flux_v[at][:, :HALF])
            )
        middle = jnp.zeros((GRID - 2 * BAND, HALF), f32)
        change_re = jnp.concatenate([push_re[0], middle, push_re[1]], axis=0)
        change_im = jnp.concatenate([push_im[0], middle, push_im[1]], axis=0)
        final = synthesize(
            base + 2,
            (real + change_re) * decay * weight,
            (imag + change_im) * decay * weight,
        )
        gap = final - target
        score = jnp.sum(gap * gap, keepdims=True) * (
            1.0 / (2.0 * noise_level * noise_level * GRID * GRID)
        )
        scores = jnp.where(lanes((1, MOVES)) == move, score, scores)
    misfit_ref[...] = scores
    out_copy.wait()


def body(particles, offspring, noise, accept, observed):
    devices = RING * PLANE
    rings = [[z * PLANE + at for z in range(RING)] for at in range(PLANE)]
    planes = [[z * PLANE + at for at in range(PLANE)] for z in range(RING)]
    vmem, smem = pl.BlockSpec(memory_space=pltpu.VMEM), pl.BlockSpec(memory_space=pltpu.SMEM)
    anywhere = pl.BlockSpec(memory_space=pl.ANY)

    def gather(tiles, groups):
        return lax.all_to_all(tiles, "dom", 0, 0, axis_index_groups=groups, tiled=True)

    def send(value, target):
        pairs = [(i, target(i)) for i in range(devices) if 0 <= target(i) < devices]
        return lax.ppermute(value, "dom", pairs)

    slot_at = lambda: lax.axis_index("dom")
    tile = pl.pallas_call(
        functools.partial(first_kernel, lambda: lax.rem(slot_at(), PLANE)),
        in_specs=[vmem, anywhere],
        out_specs=vmem,
        out_shape=jax.ShapeDtypeStruct((PLANE, 8, 128), f32),
        scratch_shapes=[
            pltpu.VMEM((2, 2, 8, HALF), f32),
            pltpu.SemaphoreType.DMA((2,)),
        ],
        compiler_params=pltpu.CompilerParams(vmem_limit_bytes=2 * 1024 * 1024),
        name="first",
    )(
        jnp.broadcast_to(offspring.astype(f32), (8, 128)),
        pltpu.with_memory_space_constraint(particles, pltpu.HBM),
    )
    behind = send(particles, lambda i: i + 2)
    ahead = send(particles, lambda i: i - 2)
    partner = send(particles, lambda i: i ^ 1)
    far = send(particles, lambda i: i + 3 if i % 2 else i - 3)
    plane = gather(tile, planes)
    tile = pl.pallas_call(
        second_kernel,
        in_specs=[vmem],
        out_specs=vmem,
        out_shape=jax.ShapeDtypeStruct((RING, 8, 128), f32),
        compiler_params=pltpu.CompilerParams(vmem_limit_bytes=2 * 1024 * 1024),
        name="second",
    )(plane)
    partner_behind = send(behind, lambda i: i ^ 1)
    partner_ahead = send(ahead, lambda i: i ^ 1)
    tiles = gather(tile, rings)
    moved, misfit = pl.pallas_call(
        functools.partial(final_kernel, slot_at),
        in_specs=[smem, vmem] + [anywhere] * 7 + [vmem] + [anywhere] * 2,
        out_specs=[anywhere, vmem],
        out_shape=[
            jax.ShapeDtypeStruct((1, 2, GRID, HALF), f32),
            jax.ShapeDtypeStruct((1, MOVES), f32),
        ],
        scratch_shapes=[
            pltpu.VMEM((2, GRID, HALF), f32),
            pltpu.VMEM((2, GRID, HALF), f32),
            pltpu.VMEM((6, GRID, GRID), bf16),
            pltpu.VMEM((6, GRID, GRID), bf16),
            pltpu.VMEM((GRID, 8 * GRID), bf16),
            pltpu.VMEM((GRID, GRID), f32),
            pltpu.SemaphoreType.DMA,
            pltpu.SemaphoreType.DMA,
            pltpu.SemaphoreType.DMA,
            pltpu.SemaphoreType.DMA,
        ],
        compiler_params=pltpu.CompilerParams(vmem_limit_bytes=24 * 1024 * 1024),
        name="final",
    )(
        accept.reshape(MOVES),
        tiles,
        particles,
        behind,
        ahead,
        partner,
        far,
        partner_behind,
        partner_ahead,
        noise,
        pltpu.with_memory_space_constraint(observed, pltpu.HBM),
        pltpu.with_memory_space_constraint(jnp.asarray(tables()), pltpu.HBM),
    )
    return moved, misfit.reshape(MOVES, 1)


def solution(mesh):
    return jax.shard_map(
        body,
        mesh=mesh,
        in_specs=(
            P("dom", None, None, None),
            P("dom"),
            P(None, "dom", None, None, None),
            P(None, "dom"),
            P(),
        ),
        out_specs=(P("dom", None, None, None), P(None, "dom")),
        check_vma=False,
    )
```

```python
import functools
import math

import jax
import jax.numpy as jnp
import numpy as np
from jax import lax
from jax.experimental import pallas as pl
from jax.experimental.pallas import tpu as pltpu
from jax.sharding import PartitionSpec as P

MOVES = 2
LOW = 16
GRID = 256
HALF = 128
CUT = GRID // 3
BAND = 96
RING = 16
PLANE = 32
COUNTS = 64

time_step = 0.05
viscosity = 0.001
noise_level = 0.5
prior_amplitude = 1.5
step_size = 0.4
keep = math.sqrt(1.0 - step_size * step_size)

f32 = jnp.float32
bf16 = jnp.bfloat16


def split_table(table):
    high = table.astype(bf16)
    low = (table - high.astype(np.float64)).astype(bf16)
    return high, low


@functools.lru_cache(maxsize=1)
def tables():
    index = np.arange(GRID)
    phase = (index[:, None] * index[None, :] % GRID) * (2.0 * np.pi / GRID)
    cos, sin = np.cos(phase), np.sin(phase)
    turned = sin[:HALF].copy()
    turned[0] = 1.0 - 2.0 * (index % 2)
    across = np.concatenate([cos[:HALF], turned], axis=0)
    down = np.concatenate([cos[:HALF], -sin[:HALF]], axis=0)
    back = np.concatenate([cos[:, :HALF], sin[:, :HALF]], axis=1)
    parts = [half for t in (across, down, back, across.T) for half in split_table(t)]
    return np.concatenate(parts, axis=1)


@functools.lru_cache(maxsize=1)
def waves():
    row, wave_x = np.arange(GRID)[:, None], np.arange(HALF)[None, :]
    wave_y = np.where(row < GRID // 2, row, row - GRID)
    wave_sq = (wave_y * wave_y + wave_x * wave_x).astype(np.float64)
    inverse_sq = np.where(wave_sq > 0, 1.0 / np.maximum(wave_sq, 1.0), 0.0)
    low = (wave_x < LOW) & ((row < LOW // 2) | (row >= GRID - LOW // 2))
    prior = prior_amplitude / (1.0 + np.sqrt(wave_sq) / 8.0)
    weight = np.where(wave_x == 0, 1.0, 2.0) / 64.0
    pull = ((np.abs(wave_y) <= CUT) & (wave_x <= CUT)) * (time_step * 64.0 / (GRID * GRID))
    return np.stack(
        [
            step_size * np.where(low, 1.0, prior),
            wave_y * inverse_sq,
            wave_x * inverse_sq,
            weight / (1.0 + time_step * viscosity * wave_sq),
            pull * wave_x,
            pull * wave_y,
        ]
    ).astype(np.float32)


def lanes(shape):
    return lax.broadcasted_iota(jnp.int32, shape, len(shape) - 1)


def first_kernel(plane_at, offspring_ref, particle_ref, tile_ref, low_buf, sems):
    copies = [
        pltpu.make_async_copy(
            particle_ref.at[0, :, pl.ds(start, 8)], low_buf.at[side], sems.at[side]
        )
        for side, start in enumerate((0, GRID - 8))
    ]
    for copy in copies:
        copy.start()
    for copy in copies:
        copy.wait()
    count = offspring_ref[...]
    lane = lanes((8, 128))
    tile = jnp.where(lane == COUNTS + plane_at(), count, 0.0)
    for part in range(2):
        for side in range(2):
            low = jnp.where(lane < LOW, low_buf[side, part], 0.0)
            square = count * (low * low)
            shift = (2 * part + side) * LOW
            tile += pltpu.roll(square, shift, 1) if shift else square
    tile_ref[...] = jnp.broadcast_to(tile[None], tile_ref.shape)


def pack_kernel(odd_at, own_ref, behind_ref, ahead_ref, pack_ref, pass_ref, sems):
    copies = [
        pltpu.make_async_copy(ref.at[0], pack_ref.at[at], sems.at[at])
        for at, ref in enumerate((own_ref, behind_ref, ahead_ref))
    ]
    for copy in copies:
        copy.start()
    odd = odd_at()
    for at, ref in enumerate((ahead_ref, behind_ref)):

        @pl.when(odd == at)
        def _(ref=ref):
            pltpu.make_async_copy(ref, pass_ref, sems.at[3]).start()

    pltpu.make_async_copy(behind_ref, pass_ref, sems.at[3]).wait()
    for copy in copies:
        copy.wait()


def second_kernel(tiles_ref, tile_ref):
    total = tiles_ref[0]
    for at in range(1, PLANE):
        total += tiles_ref[at]
    tile_ref[...] = jnp.broadcast_to(total[None], tile_ref.shape)


def split(value):
    high = value.astype(bf16)
    return high, (value - high.astype(f32)).astype(bf16)


def backwards(rows):
    count, width = rows.shape
    groups = pltpu.roll(rows, count - 1, 0).reshape(count // 8, 8, width)
    sub = lax.broadcasted_iota(jnp.int32, groups.shape, 1)
    for step in (4, 2, 1):
        up, lower = pltpu.roll(groups, 8 - step, 1), pltpu.roll(groups, step, 1)
        groups = jnp.where(lax.rem(lax.div(sub, step), 2) == 0, up, lower)
    return jnp.concatenate([groups[i] for i in range(count // 8)][::-1], axis=0)


def product(left_high, left_low, right_high, right_low):
    dot = functools.partial(jnp.dot, preferred_element_type=f32)
    return (
        dot(left_high, right_high) + dot(left_low, right_high) + dot(left_high, right_low)
    )


def final_kernel(
    slot_at,
    accept_hbm,
    tiles_ref,
    near_ref,
    far_ref,
    partner_ref,
    noise_ref,
    observed_hbm,
    waves_hbm,
    table_hbm,
    moved_ref,
    misfit_ref,
    chosen,
    moved_buf,
    data_high,
    data_low,
    accept_ref,
    observed_ref,
    waves_ref,
    table_buf,
    sems,
    in_sem,
    out_sem,
):
    loads = [
        pltpu.make_async_copy(source, target, sems.at[at])
        for at, (source, target) in enumerate(
            (
                (accept_hbm, accept_ref),
                (waves_hbm.at[:3], waves_ref.at[:3]),
                (table_hbm.at[:, : 2 * GRID], table_buf.at[:, : 2 * GRID]),
                (table_hbm.at[:, 2 * GRID : 4 * GRID], table_buf.at[:, 2 * GRID : 4 * GRID]),
                (table_hbm.at[:, 4 * GRID :], table_buf.at[:, 4 * GRID :]),
                (waves_hbm.at[3:], waves_ref.at[3:]),
                (observed_hbm, observed_ref),
            )
        )
    ]
    for load in loads:
        load.start()
    across, down, back, gather = (
        [table_buf.at[:, start : start + GRID] for start in (at, at + GRID)]
        for at in range(0, 8 * GRID, 2 * GRID)
    )
    slot = slot_at()
    odd = lax.rem(slot, 2)

    counts = tiles_ref[:, 0, :]
    lane = lanes((RING, 128))
    ring_at = lax.broadcasted_iota(jnp.int32, (RING, 128), 0)
    place = ring_at * PLANE + lane - COUNTS
    counted = (lane >= COUNTS) & (lane < COUNTS + PLANE)
    offset = jnp.full((1, 1), -3, jnp.int32)
    for distance in range(-3, 4):
        ends = jnp.sum(
            jnp.where(counted & (place <= slot + distance), counts, 0.0), keepdims=True
        )
        offset += (ends <= slot.astype(f32)).astype(jnp.int32)
    offset = jnp.minimum(offset, 3)[0, 0]

    side = 1 - 2 * odd
    here = lax.rem(offset + 4, 2) == 0
    far = offset == -3 * side
    step = offset - jnp.where(here, 0, side)
    at = jnp.where(step == 0, 0, jnp.where(step < 0, 1, 2))

    @pl.when(here)
    def _():
        pltpu.make_async_copy(near_ref.at[at], chosen, in_sem).start()

    @pl.when(far)
    def _():
        pltpu.make_async_copy(far_ref.at[0], chosen, in_sem).start()

    @pl.when(jnp.logical_not(here | far))
    def _():
        pltpu.make_async_copy(partner_ref.at[at], chosen, in_sem).start()

    along, cross, damped = (waves_ref.at[i] for i in range(1, 4))
    weight = jnp.where(lanes((1, HALF)) == 0, 1.0 / 64, 2.0 / 64)

    total = tiles_ref[0]
    for at in range(1, RING):
        total += tiles_ref[at]
    adapted = jnp.sqrt(jnp.maximum(total, 0.0) / (RING * PLANE) + 1e-06)
    low_lane = lanes((8, HALF)) < LOW

    factors = [
        jnp.where(low_lane, pltpu.roll(adapted, (128 - at * LOW) % 128, 1) if at else adapted, 1.0)
        for at in range(4)
    ]

    def kick(move, part):
        value = waves_ref[0] * noise_ref[move, 0, part]
        return jnp.concatenate(
            [
                value[:8] * factors[2 * part],
                value[8 : GRID - 8],
                value[GRID - 8 :] * factors[2 * part + 1],
            ],
            axis=0,
        )

    loads[0].wait()
    loads[1].wait()
    pltpu.make_async_copy(far_ref.at[0], chosen, in_sem).wait()
    current = [chosen[part] for part in range(2)]
    proposals = []
    for move in range(MOVES):
        proposal = [keep * current[part] + kick(move, part) for part in range(2)]
        proposals.append(proposal)
        taken = accept_ref[move] == 1
        current = [jnp.where(taken, proposal[part], current[part]) for part in range(2)]
    for part in range(2):
        moved_buf[part] = current[part]
    out_copy = pltpu.make_async_copy(moved_buf, moved_ref.at[0], out_sem)
    out_copy.start()


    def synthesize(at, real, imag):
        for half, value in enumerate((real, imag)):
            high, low = split(value)
            data_high[at, :, half * HALF : (half + 1) * HALF] = high
            data_low[at, :, half * HALF : (half + 1) * HALF] = low
        both = product(across[0][...], across[1][...], data_high[at], data_low[at])
        even_re, even_im = both[:HALF, :HALF], both[:HALF, HALF:]
        odd_re, odd_im = both[HALF:, :HALF], both[HALF:, HALF:]
        rows_re = jnp.concatenate(
            [
                jnp.where(first_row, even_re, even_re - odd_im),
                jnp.where(first_row, odd_re, even_re + odd_im),
            ],
            axis=0,
        )
        rows_im = jnp.concatenate(
            [
                jnp.where(first_row, even_im, even_im + odd_re),
                jnp.where(first_row, odd_im, even_im - odd_re),
            ],
            axis=0,
        )
        rows = jnp.concatenate([rows_re, rows_im], axis=1)
        return product(*split(rows), down[0][...], down[1][...])

    def analyse(at, field):
        rows = product(*split(field), back[0][...], back[1][...])
        plus_c, plus_s = rows[:HALF, :HALF], rows[:HALF, HALF:]
        minus_c, minus_s = rows[HALF:, :HALF], rows[HALF:, HALF:]
        quarters = (
            (0, 0, jnp.where(first_row, plus_c, plus_c + minus_c)),
            (0, HALF, -jnp.where(first_row, plus_s, plus_s + minus_s)),
            (HALF, 0, jnp.where(first_row, minus_c, minus_s - plus_s)),
            (HALF, HALF, jnp.where(first_row, -minus_s, minus_c - plus_c)),
        )
        for row, column, value in quarters:
            high, low = split(value)
            data_high[at, row : row + HALF, column : column + HALF] = high
            data_low[at, row : row + HALF, column : column + HALF] = low
        return [
            product(
                gather[0][start : start + BAND],
                gather[1][start : start + BAND],
                data_high[at],
                data_low[at],
            )
            for start in (0, GRID - BAND)
        ]

    first_row = lax.broadcasted_iota(jnp.int32, (HALF, HALF), 0) == 0
    loads[2].wait()
    loads[3].wait()
    fields = []
    for move in range(MOVES):
        wr, wi = (value * weight for value in proposals[move])
        fields.append(
            (
                synthesize(3 * move, wr, wi),
                synthesize(3 * move + 1, -along[...] * wi, along[...] * wr),
                synthesize(3 * move + 2, cross[...] * wi, -cross[...] * wr),
            )
        )
    for load in loads[4:]:
        load.wait()
    fluxes = [
        (analyse(6 + 2 * move, flow_u * vort), analyse(7 + 2 * move, flow_v * vort))
        for move, (vort, flow_u, flow_v) in enumerate(fields)
    ]
    finals = []
    for move, (flux_u, flux_v) in enumerate(fluxes):
        bands = []
        for at, start in enumerate((0, GRID - BAND)):
            kx, ky = (waves_ref[i, start : start + BAND] for i in (4, 5))
            push = kx * flux_u[at][:, HALF:] + ky * flux_v[at][:, HALF:]
            lift = kx * flux_u[at][:, :HALF] + ky * flux_v[at][:, :HALF]
            bands.append((push, lift))
        middle = jnp.zeros((GRID - 2 * BAND, HALF), f32)
        change_re, change_im = (
            jnp.concatenate([bands[0][i], middle, bands[1][i]], axis=0) for i in range(2)
        )
        real, imag = proposals[move]
        finals.append(
            synthesize(
                10 + move, (real + change_re) * damped[...], (imag - change_im) * damped[...]
            )
        )
    target = jnp.concatenate(
        [observed_ref[:HALF], backwards(observed_ref[HALF:])], axis=0
    )
    scores = jnp.zeros((1, MOVES), f32)
    for move, final in enumerate(finals):
        gap = final - target
        score = jnp.sum(gap * gap, keepdims=True) * (
            1.0 / (2.0 * noise_level * noise_level * GRID * GRID)
        )
        scores = jnp.where(lanes((1, MOVES)) == move, score, scores)
    misfit_ref[...] = scores
    out_copy.wait()


def body(particles, offspring, noise, accept, observed):
    devices = RING * PLANE
    rings = [[z * PLANE + at for z in range(RING)] for at in range(PLANE)]
    planes = [[z * PLANE + at for at in range(PLANE)] for z in range(RING)]
    vmem, smem = pl.BlockSpec(memory_space=pltpu.VMEM), pl.BlockSpec(memory_space=pltpu.SMEM)
    anywhere = pl.BlockSpec(memory_space=pl.ANY)

    def gather(tiles, groups):
        return lax.all_to_all(tiles, "dom", 0, 0, axis_index_groups=groups, tiled=True)

    def send(value, target):
        pairs = [(i, target(i)) for i in range(devices) if 0 <= target(i) < devices]
        return lax.ppermute(value, "dom", pairs)

    in_hbm = functools.partial(pltpu.with_memory_space_constraint, memory_space=pltpu.HBM)
    slot_at = lambda: lax.axis_index("dom")
    tile = pl.pallas_call(
        functools.partial(first_kernel, lambda: lax.rem(slot_at(), PLANE)),
        in_specs=[vmem, anywhere],
        out_specs=vmem,
        out_shape=jax.ShapeDtypeStruct((PLANE, 8, 128), f32),
        scratch_shapes=[
            pltpu.VMEM((2, 2, 8, HALF), f32),
            pltpu.SemaphoreType.DMA((2,)),
        ],
        compiler_params=pltpu.CompilerParams(vmem_limit_bytes=2 * 1024 * 1024),
        name="first",
    )(
        jnp.broadcast_to(offspring.astype(f32), (8, 128)),
        pltpu.with_memory_space_constraint(particles, pltpu.HBM),
    )
    behind = send(particles, lambda i: i + 2)
    ahead = send(particles, lambda i: i - 2)
    plane = gather(tile, planes)
    tile = pl.pallas_call(
        second_kernel,
        in_specs=[vmem],
        out_specs=vmem,
        out_shape=jax.ShapeDtypeStruct((RING, 8, 128), f32),
        compiler_params=pltpu.CompilerParams(vmem_limit_bytes=2 * 1024 * 1024),
        name="second",
    )(plane)
    packed, passed = pl.pallas_call(
        functools.partial(pack_kernel, lambda: lax.rem(slot_at(), 2)),
        in_specs=[anywhere] * 3,
        out_specs=[anywhere] * 2,
        out_shape=[
            jax.ShapeDtypeStruct((3, 2, GRID, HALF), f32),
            jax.ShapeDtypeStruct((1, 2, GRID, HALF), f32),
        ],
        scratch_shapes=[pltpu.SemaphoreType.DMA((4,))],
        compiler_params=pltpu.CompilerParams(vmem_limit_bytes=2 * 1024 * 1024),
        name="pack",
    )(particles, behind, ahead)
    far = send(passed, lambda i: i + 1 if i % 2 else i - 1)
    partner = send(packed, lambda i: i ^ 1)
    tiles = gather(tile, rings)
    moved, misfit = pl.pallas_call(
        functools.partial(final_kernel, slot_at),
        in_specs=[anywhere, vmem] + [anywhere] * 3 + [vmem] + [anywhere] * 3,
        out_specs=[anywhere, vmem],
        out_shape=[
            jax.ShapeDtypeStruct((1, 2, GRID, HALF), f32),
            jax.ShapeDtypeStruct((1, MOVES), f32),
        ],
        scratch_shapes=[
            pltpu.VMEM((2, GRID, HALF), f32),
            pltpu.VMEM((2, GRID, HALF), f32),
            pltpu.VMEM((12, GRID, GRID), bf16),
            pltpu.VMEM((12, GRID, GRID), bf16),
            pltpu.SMEM((MOVES,), jnp.int32),
            pltpu.VMEM((GRID, GRID), f32),
            pltpu.VMEM((6, GRID, HALF), f32),
            pltpu.VMEM((GRID, 8 * GRID), bf16),
            pltpu.SemaphoreType.DMA((7,)),
            pltpu.SemaphoreType.DMA,
            pltpu.SemaphoreType.DMA,
        ],
        compiler_params=pltpu.CompilerParams(vmem_limit_bytes=24 * 1024 * 1024),
        name="final",
    )(
        in_hbm(accept.reshape(MOVES)),
        tiles,
        packed,
        far,
        partner,
        noise,
        in_hbm(observed),
        in_hbm(jnp.asarray(waves())),
        in_hbm(jnp.asarray(tables())),
    )
    return moved, misfit.reshape(MOVES, 1)


def solution(mesh):
    return jax.shard_map(
        body,
        mesh=mesh,
        in_specs=(
            P("dom", None, None, None),
            P("dom"),
            P(None, "dom", None, None, None),
            P(None, "dom"),
            P(),
        ),
        out_specs=(P("dom", None, None, None), P(None, "dom")),
        check_vma=False,
    )
```

```python
import functools
import math

import jax
import jax.numpy as jnp
import numpy as np
from jax import lax
from jax.experimental import pallas as pl
from jax.experimental.pallas import tpu as pltpu
from jax.sharding import PartitionSpec as P

MOVES = 2
LOW = 16
GRID = 256
HALF = 128
CUT = GRID // 3
BAND = 96
RING = 16
PLANE = 32
COUNTS = 64

time_step = 0.05
viscosity = 0.001
noise_level = 0.5
prior_amplitude = 1.5
step_size = 0.4
keep = math.sqrt(1.0 - step_size * step_size)

f32 = jnp.float32
bf16 = jnp.bfloat16


def split_table(table):
    high = table.astype(bf16)
    low = (table - high.astype(np.float64)).astype(bf16)
    return high, low


@functools.lru_cache(maxsize=1)
def tables():
    index = np.arange(GRID)
    phase = (index[:, None] * index[None, :] % GRID) * (2.0 * np.pi / GRID)
    cos, sin = np.cos(phase), np.sin(phase)
    turned = sin[:HALF].copy()
    turned[0] = 1.0 - 2.0 * (index % 2)
    across = np.concatenate([cos[:HALF], turned], axis=0)
    down = np.concatenate([cos[:HALF], -sin[:HALF]], axis=0)
    back = np.concatenate([cos[:, :HALF], sin[:, :HALF]], axis=1)
    parts = [half for t in (across, down, back, across.T) for half in split_table(t)]
    return np.concatenate(parts, axis=1)


@functools.lru_cache(maxsize=1)
def waves():
    row, wave_x = np.arange(GRID)[:, None], np.arange(HALF)[None, :]
    wave_y = np.where(row < GRID // 2, row, row - GRID)
    wave_sq = (wave_y * wave_y + wave_x * wave_x).astype(np.float64)
    inverse_sq = np.where(wave_sq > 0, 1.0 / np.maximum(wave_sq, 1.0), 0.0)
    low = (wave_x < LOW) & ((row < LOW // 2) | (row >= GRID - LOW // 2))
    prior = prior_amplitude / (1.0 + np.sqrt(wave_sq) / 8.0)
    weight = np.where(wave_x == 0, 1.0, 2.0) / 64.0
    pull = ((np.abs(wave_y) <= CUT) & (wave_x <= CUT)) * (time_step * 64.0 / (GRID * GRID))
    return np.stack(
        [
            step_size * np.where(low, 1.0, prior),
            wave_y * inverse_sq,
            wave_x * inverse_sq,
            weight / (1.0 + time_step * viscosity * wave_sq),
            pull * wave_x,
            pull * wave_y,
        ]
    ).astype(np.float32)


def lanes(shape):
    return lax.broadcasted_iota(jnp.int32, shape, len(shape) - 1)


def first_kernel(plane_at, offspring_ref, particle_ref, tile_ref, low_buf, sems):
    copies = [
        pltpu.make_async_copy(
            particle_ref.at[0, :, pl.ds(start, 8)], low_buf.at[side], sems.at[side]
        )
        for side, start in enumerate((0, GRID - 8))
    ]
    for copy in copies:
        copy.start()
    for copy in copies:
        copy.wait()
    count = offspring_ref[...]
    lane = lanes((8, 128))
    tile = jnp.where(lane == COUNTS + plane_at(), count, 0.0)
    for part in range(2):
        for side in range(2):
            low = jnp.where(lane < LOW, low_buf[side, part], 0.0)
            square = count * (low * low)
            shift = (2 * part + side) * LOW
            tile += pltpu.roll(square, shift, 1) if shift else square
    tile_ref[...] = jnp.broadcast_to(tile[None], tile_ref.shape)


def pack_kernel(own_ref, behind_ref, ahead_ref, pack_ref, sems):
    copies = [
        pltpu.make_async_copy(ref.at[0], pack_ref.at[at], sems.at[at])
        for at, ref in enumerate((own_ref, behind_ref, ahead_ref))
    ]
    for copy in copies:
        copy.start()
    for copy in copies:
        copy.wait()


def second_kernel(tiles_ref, tile_ref):
    total = tiles_ref[0]
    for at in range(1, PLANE):
        total += tiles_ref[at]
    tile_ref[...] = jnp.broadcast_to(total[None], tile_ref.shape)


def split(value):
    high = value.astype(bf16)
    return high, (value - high.astype(f32)).astype(bf16)


def backwards(rows):
    count, width = rows.shape
    groups = pltpu.roll(rows, count - 1, 0).reshape(count // 8, 8, width)
    sub = lax.broadcasted_iota(jnp.int32, groups.shape, 1)
    for step in (4, 2, 1):
        up, lower = pltpu.roll(groups, 8 - step, 1), pltpu.roll(groups, step, 1)
        groups = jnp.where(lax.rem(lax.div(sub, step), 2) == 0, up, lower)
    return jnp.concatenate([groups[i] for i in range(count // 8)][::-1], axis=0)


def product(left_high, left_low, right_high, right_low):
    dot = functools.partial(jnp.dot, preferred_element_type=f32)
    return (
        dot(left_high, right_high) + dot(left_low, right_high) + dot(left_high, right_low)
    )


def final_kernel(
    slot_at,
    accept_hbm,
    tiles_ref,
    near_ref,
    far_ref,
    partner_ref,
    noise_ref,
    observed_hbm,
    waves_hbm,
    table_hbm,
    moved_ref,
    misfit_ref,
    chosen,
    moved_buf,
    data_high,
    data_low,
    accept_ref,
    observed_ref,
    waves_ref,
    table_buf,
    sems,
    in_sem,
    out_sem,
):
    loads = [
        pltpu.make_async_copy(source, target, sems.at[at])
        for at, (source, target) in enumerate(
            (
                (accept_hbm, accept_ref),
                (waves_hbm.at[:3], waves_ref.at[:3]),
                (table_hbm.at[:, : 2 * GRID], table_buf.at[:, : 2 * GRID]),
                (table_hbm.at[:, 2 * GRID : 4 * GRID], table_buf.at[:, 2 * GRID : 4 * GRID]),
                (table_hbm.at[:, 4 * GRID :], table_buf.at[:, 4 * GRID :]),
                (waves_hbm.at[3:], waves_ref.at[3:]),
                (observed_hbm, observed_ref),
            )
        )
    ]
    for load in loads:
        load.start()
    across, down, back, gather = (
        [table_buf.at[:, start : start + GRID] for start in (at, at + GRID)]
        for at in range(0, 8 * GRID, 2 * GRID)
    )
    slot = slot_at()
    odd = lax.rem(slot, 2)

    counts = tiles_ref[:, 0, :]
    lane = lanes((RING, 128))
    ring_at = lax.broadcasted_iota(jnp.int32, (RING, 128), 0)
    place = ring_at * PLANE + lane - COUNTS
    counted = (lane >= COUNTS) & (lane < COUNTS + PLANE)
    offset = jnp.full((1, 1), -3, jnp.int32)
    for distance in range(-3, 4):
        ends = jnp.sum(
            jnp.where(counted & (place <= slot + distance), counts, 0.0), keepdims=True
        )
        offset += (ends <= slot.astype(f32)).astype(jnp.int32)
    offset = jnp.minimum(offset, 3)[0, 0]

    side = 1 - 2 * odd
    here = lax.rem(offset + 4, 2) == 0
    far = offset == -3 * side
    step = offset - jnp.where(here, 0, side)
    at = jnp.where(step == 0, 0, jnp.where(step < 0, 1, 2))

    @pl.when(here)
    def _():
        pltpu.make_async_copy(near_ref.at[at], chosen, in_sem).start()

    @pl.when(far)
    def _():
        pltpu.make_async_copy(far_ref.at[0], chosen, in_sem).start()

    @pl.when(jnp.logical_not(here | far))
    def _():
        pltpu.make_async_copy(partner_ref.at[at], chosen, in_sem).start()

    along, cross, damped = (waves_ref.at[i] for i in range(1, 4))
    weight = jnp.where(lanes((1, HALF)) == 0, 1.0 / 64, 2.0 / 64)

    total = tiles_ref[0]
    for at in range(1, RING):
        total += tiles_ref[at]
    adapted = jnp.sqrt(jnp.maximum(total, 0.0) / (RING * PLANE) + 1e-06)
    low_lane = lanes((8, HALF)) < LOW

    factors = [
        jnp.where(low_lane, pltpu.roll(adapted, (128 - at * LOW) % 128, 1) if at else adapted, 1.0)
        for at in range(4)
    ]

    def kick(move, part):
        value = waves_ref[0] * noise_ref[move, 0, part]
        return jnp.concatenate(
            [
                value[:8] * factors[2 * part],
                value[8 : GRID - 8],
                value[GRID - 8 :] * factors[2 * part + 1],
            ],
            axis=0,
        )

    loads[0].wait()
    loads[1].wait()
    pltpu.make_async_copy(far_ref.at[0], chosen, in_sem).wait()
    current = [chosen[part] for part in range(2)]
    proposals = []
    for move in range(MOVES):
        proposal = [keep * current[part] + kick(move, part) for part in range(2)]
        proposals.append(proposal)
        taken = accept_ref[move] == 1
        current = [jnp.where(taken, proposal[part], current[part]) for part in range(2)]
    for part in range(2):
        moved_buf[part] = current[part]
    out_copy = pltpu.make_async_copy(moved_buf, moved_ref.at[0], out_sem)
    out_copy.start()


    def synthesize(at, real, imag):
        for half, value in enumerate((real, imag)):
            high, low = split(value)
            data_high[at, :, half * HALF : (half + 1) * HALF] = high
            data_low[at, :, half * HALF : (half + 1) * HALF] = low
        both = product(across[0][...], across[1][...], data_high[at], data_low[at])
        even_re, even_im = both[:HALF, :HALF], both[:HALF, HALF:]
        odd_re, odd_im = both[HALF:, :HALF], both[HALF:, HALF:]
        rows_re = jnp.concatenate(
            [
                jnp.where(first_row, even_re, even_re - odd_im),
                jnp.where(first_row, odd_re, even_re + odd_im),
            ],
            axis=0,
        )
        rows_im = jnp.concatenate(
            [
                jnp.where(first_row, even_im, even_im + odd_re),
                jnp.where(first_row, odd_im, even_im - odd_re),
            ],
            axis=0,
        )
        rows = jnp.concatenate([rows_re, rows_im], axis=1)
        return product(*split(rows), down[0][...], down[1][...])

    def analyse(at, field):
        rows = product(*split(field), back[0][...], back[1][...])
        plus_c, plus_s = rows[:HALF, :HALF], rows[:HALF, HALF:]
        minus_c, minus_s = rows[HALF:, :HALF], rows[HALF:, HALF:]
        quarters = (
            (0, 0, jnp.where(first_row, plus_c, plus_c + minus_c)),
            (0, HALF, -jnp.where(first_row, plus_s, plus_s + minus_s)),
            (HALF, 0, jnp.where(first_row, minus_c, minus_s - plus_s)),
            (HALF, HALF, jnp.where(first_row, -minus_s, minus_c - plus_c)),
        )
        for row, column, value in quarters:
            high, low = split(value)
            data_high[at, row : row + HALF, column : column + HALF] = high
            data_low[at, row : row + HALF, column : column + HALF] = low
        return [
            product(
                gather[0][start : start + BAND],
                gather[1][start : start + BAND],
                data_high[at],
                data_low[at],
            )
            for start in (0, GRID - BAND)
        ]

    first_row = lax.broadcasted_iota(jnp.int32, (HALF, HALF), 0) == 0
    loads[2].wait()
    loads[3].wait()
    fields = []
    for move in range(MOVES):
        wr, wi = (value * weight for value in proposals[move])
        fields.append(
            (
                synthesize(3 * move, wr, wi),
                synthesize(3 * move + 1, -along[...] * wi, along[...] * wr),
                synthesize(3 * move + 2, cross[...] * wi, -cross[...] * wr),
            )
        )
    for load in loads[4:]:
        load.wait()
    fluxes = [
        (analyse(6 + 2 * move, flow_u * vort), analyse(7 + 2 * move, flow_v * vort))
        for move, (vort, flow_u, flow_v) in enumerate(fields)
    ]
    finals = []
    for move, (flux_u, flux_v) in enumerate(fluxes):
        bands = []
        for at, start in enumerate((0, GRID - BAND)):
            kx, ky = (waves_ref[i, start : start + BAND] for i in (4, 5))
            push = kx * flux_u[at][:, HALF:] + ky * flux_v[at][:, HALF:]
            lift = kx * flux_u[at][:, :HALF] + ky * flux_v[at][:, :HALF]
            bands.append((push, lift))
        middle = jnp.zeros((GRID - 2 * BAND, HALF), f32)
        change_re, change_im = (
            jnp.concatenate([bands[0][i], middle, bands[1][i]], axis=0) for i in range(2)
        )
        real, imag = proposals[move]
        finals.append(
            synthesize(
                10 + move, (real + change_re) * damped[...], (imag - change_im) * damped[...]
            )
        )
    target = jnp.concatenate(
        [observed_ref[:HALF], backwards(observed_ref[HALF:])], axis=0
    )
    scores = jnp.zeros((1, MOVES), f32)
    for move, final in enumerate(finals):
        gap = final - target
        score = jnp.sum(gap * gap, keepdims=True) * (
            1.0 / (2.0 * noise_level * noise_level * GRID * GRID)
        )
        scores = jnp.where(lanes((1, MOVES)) == move, score, scores)
    misfit_ref[...] = scores
    out_copy.wait()


def body(particles, offspring, noise, accept, observed):
    devices = RING * PLANE
    rings = [[z * PLANE + at for z in range(RING)] for at in range(PLANE)]
    planes = [[z * PLANE + at for at in range(PLANE)] for z in range(RING)]
    vmem, smem = pl.BlockSpec(memory_space=pltpu.VMEM), pl.BlockSpec(memory_space=pltpu.SMEM)
    anywhere = pl.BlockSpec(memory_space=pl.ANY)

    def gather(tiles, groups):
        return lax.all_to_all(tiles, "dom", 0, 0, axis_index_groups=groups, tiled=True)

    def send(value, target):
        pairs = [(i, target(i)) for i in range(devices) if 0 <= target(i) < devices]
        return lax.ppermute(value, "dom", pairs)

    in_hbm = functools.partial(pltpu.with_memory_space_constraint, memory_space=pltpu.HBM)
    slot_at = lambda: lax.axis_index("dom")
    tile = pl.pallas_call(
        functools.partial(first_kernel, lambda: lax.rem(slot_at(), PLANE)),
        in_specs=[vmem, anywhere],
        out_specs=vmem,
        out_shape=jax.ShapeDtypeStruct((PLANE, 8, 128), f32),
        scratch_shapes=[
            pltpu.VMEM((2, 2, 8, HALF), f32),
            pltpu.SemaphoreType.DMA((2,)),
        ],
        compiler_params=pltpu.CompilerParams(vmem_limit_bytes=2 * 1024 * 1024),
        name="first",
    )(
        jnp.broadcast_to(offspring.astype(f32), (8, 128)),
        pltpu.with_memory_space_constraint(particles, pltpu.HBM),
    )
    behind = send(particles, lambda i: i + 2)
    ahead = send(particles, lambda i: i - 2)
    plane = gather(tile, planes)
    tile = pl.pallas_call(
        second_kernel,
        in_specs=[vmem],
        out_specs=vmem,
        out_shape=jax.ShapeDtypeStruct((RING, 8, 128), f32),
        compiler_params=pltpu.CompilerParams(vmem_limit_bytes=2 * 1024 * 1024),
        name="second",
    )(plane)
    packed = pl.pallas_call(
        pack_kernel,
        in_specs=[anywhere] * 3,
        out_specs=anywhere,
        out_shape=jax.ShapeDtypeStruct((3, 2, GRID, HALF), f32),
        scratch_shapes=[pltpu.SemaphoreType.DMA((3,))],
        compiler_params=pltpu.CompilerParams(vmem_limit_bytes=2 * 1024 * 1024),
        name="pack",
    )(particles, behind, ahead)
    far = send(particles, lambda i: i + 3 if i % 2 else i - 3)
    partner = send(packed, lambda i: i ^ 1)
    tiles = gather(tile, rings)
    moved, misfit = pl.pallas_call(
        functools.partial(final_kernel, slot_at),
        in_specs=[anywhere, vmem] + [anywhere] * 3 + [vmem] + [anywhere] * 3,
        out_specs=[anywhere, vmem],
        out_shape=[
            jax.ShapeDtypeStruct((1, 2, GRID, HALF), f32),
            jax.ShapeDtypeStruct((1, MOVES), f32),
        ],
        scratch_shapes=[
            pltpu.VMEM((2, GRID, HALF), f32),
            pltpu.VMEM((2, GRID, HALF), f32),
            pltpu.VMEM((12, GRID, GRID), bf16),
            pltpu.VMEM((12, GRID, GRID), bf16),
            pltpu.SMEM((MOVES,), jnp.int32),
            pltpu.VMEM((GRID, GRID), f32),
            pltpu.VMEM((6, GRID, HALF), f32),
            pltpu.VMEM((GRID, 8 * GRID), bf16),
            pltpu.SemaphoreType.DMA((7,)),
            pltpu.SemaphoreType.DMA,
            pltpu.SemaphoreType.DMA,
        ],
        compiler_params=pltpu.CompilerParams(vmem_limit_bytes=24 * 1024 * 1024),
        name="final",
    )(
        in_hbm(accept.reshape(MOVES)),
        tiles,
        packed,
        far,
        partner,
        noise,
        in_hbm(observed),
        in_hbm(jnp.asarray(waves())),
        in_hbm(jnp.asarray(tables())),
    )
    return moved, misfit.reshape(MOVES, 1)


def solution(mesh):
    return jax.shard_map(
        body,
        mesh=mesh,
        in_specs=(
            P("dom", None, None, None),
            P("dom"),
            P(None, "dom", None, None, None),
            P(None, "dom"),
            P(),
        ),
        out_specs=(P("dom", None, None, None), P(None, "dom")),
        check_vma=False,
    )
```
